256 devices in a mesh: replica: 8 (over y, x_hi), fsdp: 32 (over z, x_lo, core).
Axes of the slice: x: 4 (x_hi: 2, x_lo: 2; x = x_hi * 2 + x_lo), y: 4, z: 8, core: 2. Of those that a mesh axis runs over, the one named last changes fastest.
Arguments:
- partner: int32 [8], replicated, may hold values from 0 to 7, as said below
- tokens: bfloat16 [8, 512, 4096], P('replica', 'fsdp'), may hold values from -6 to 6
- w_gate: bfloat16 [8, 7168, 4096], P('replica', 'fsdp'), may hold values from -0.09375 to 0.09375
- w_up: bfloat16 [8, 7168, 4096], P('replica', 'fsdp'), may hold values from -0.09375 to 0.09375
- w_down: bfloat16 [8, 7168, 4096], P('replica', 'fsdp'), may hold values from -0.0625 to 0.0625
Outputs:
- grad_gate: bfloat16 [8, 7168, 4096], P('replica', 'fsdp')
- grad_up: bfloat16 [8, 7168, 4096], P('replica', 'fsdp')
- grad_down: bfloat16 [8, 7168, 4096], P('replica', 'fsdp')
The draws below stay inside these ranges and needn't reach their ends.
Inputs may be any that keep to these rules, and one draw needn't show every extreme that they name: partner is a permutation of the 8 replicas that forms one single cycle through all of them; no replica is its own partner.
All inputs are finite; a program needn't handle non-finite values.
Results may differ from the reference program's by a relative error of at most 0.025.
Values may be sent and summed in bfloat16 or wider, within the bound.
A program may use at most 128 MiB of HBM per device.

```python
import math
import jax
import jax.numpy as jnp
from jax import lax

D = 4096
FFW = 7168
REPLICAS = 8
TOKENS = 512
BLOCKS = 32


def draw_partner(key, part):
    order = jax.random.permutation(jax.random.fold_in(key, 17), REPLICAS).astype(jnp.int32)
    following = jnp.roll(order, -1).astype(jnp.int32)
    result = jnp.zeros((REPLICAS,), jnp.int32).at[order].set(following)
    return result.astype(jnp.int32)


def level_of(own_key, extent, pieces, smallest, high):
    level = 1.0
    for position, shards_of in pieces:
        heights = jax.random.uniform(jax.random.fold_in(jax.random.fold_in(own_key, 6), position), (shards_of,), jnp.float32, smallest / len(pieces), high / len(pieces))
        level = level * jnp.repeat(jnp.exp(heights), extent[position] // shards_of).reshape((-1,) + (1,) * (len(extent) - 1 - position))
    return level


def centred(own_key, shape, spread, limit, cuts=(), dtype=jnp.bfloat16):
    drawn = jax.random.normal(own_key, shape, jnp.float32) * spread
    if len(cuts) > 0:
        drawn = level_of(own_key, shape, cuts, -0.22, 0.18) * drawn
    return jnp.clip(drawn, min=-limit, max=limit).astype(dtype)


def setup_inputs(seed: int = 0) -> dict:
    streams_of = jax.random.split(jax.random.key(seed), 6)
    return {
        "partner": draw_partner(jax.random.fold_in(streams_of[5], 71), 0),
        "tokens": centred(streams_of[1], (REPLICAS, TOKENS, D), 1.0, 6.0, ((0, 8), (1, 32))),
        "w_gate": centred(streams_of[2], (REPLICAS, FFW, D), D ** -0.5, 0.09375, ((0, 8), (1, 32))),
        "w_up": centred(streams_of[3], (REPLICAS, FFW, D), D ** -0.5, 0.09375, ((0, 8), (1, 32))),
        "w_down": centred(streams_of[4], (REPLICAS, FFW, D), FFW ** -0.5, 0.0625, ((0, 8), (1, 32))),
    }


def forward_pass(rows, gate_w, up_w, down_w):
    pre_gate = jnp.dot(rows, gate_w.T, preferred_element_type=jnp.float32)
    pre_up = jnp.dot(rows, up_w.T, preferred_element_type=jnp.float32)
    hidden = (jax.nn.silu(pre_gate) * pre_up).astype(jnp.bfloat16)
    width = FFW // BLOCKS
    hidden_blocks = hidden.reshape(TOKENS, BLOCKS, width).transpose(1, 0, 2)
    down_blocks = down_w.reshape(BLOCKS, width, D)

    def add_block(total, pair):
        term = jnp.dot(pair[0], pair[1], preferred_element_type=jnp.float32).astype(jnp.bfloat16)
        term = lax.optimization_barrier(term)
        return (total + term.astype(jnp.float32), None)
    output, _ = lax.scan(add_block, jnp.zeros((TOKENS, D), jnp.float32), (hidden_blocks, down_blocks))
    return (pre_gate, pre_up, hidden, output)

def reference(partner, tokens, w_gate, w_up, w_down):
    loss_scale = 1.0 / math.sqrt(TOKENS)
    gates_out = []
    ups_out = []
    downs_out = []
    for replica_id in range(REPLICAS):
        rows = tokens[replica_id]
        pre_gate, pre_up, hidden, student = forward_pass(rows, w_gate[replica_id], w_up[replica_id], w_down[replica_id])
        teacher_id = partner[replica_id]
        teacher_gate = jnp.take(w_gate, teacher_id, axis=0)
        teacher_up = jnp.take(w_up, teacher_id, axis=0)
        teacher_down = jnp.take(w_down, teacher_id, axis=0)
        teacher = forward_pass(rows, teacher_gate, teacher_up, teacher_down)[3]
        cotangent = ((student - teacher) * loss_scale).astype(jnp.bfloat16)
        grad_down = jnp.dot(hidden.T, cotangent, preferred_element_type=jnp.float32).astype(jnp.bfloat16)
        d_hidden = jnp.dot(cotangent, w_down[replica_id].T, preferred_element_type=jnp.float32)
        sigma = jax.nn.sigmoid(pre_gate)
        d_gate = (d_hidden * pre_up * sigma * (1.0 + pre_gate * (1.0 - sigma))).astype(jnp.bfloat16)
        d_up = (d_hidden * pre_gate * sigma).astype(jnp.bfloat16)
        grad_gate = jnp.dot(d_gate.T, rows, preferred_element_type=jnp.float32).astype(jnp.bfloat16)
        grad_up = jnp.dot(d_up.T, rows, preferred_element_type=jnp.float32).astype(jnp.bfloat16)
        gates_out.append(grad_gate)
        ups_out.append(grad_up)
        downs_out.append(grad_down)
    return (jnp.stack(gates_out), jnp.stack(ups_out), jnp.stack(downs_out))
```

```python
import functools
import math

import jax
import jax.numpy as jnp
from jax import lax
from jax.experimental import pallas as pl
from jax.experimental.pallas import tpu as pltpu
from jax.sharding import Mesh
from jax.sharding import PartitionSpec as P

MESH = pl.DeviceIdType.MESH
REPLICA = ("ry", "rx")
FSDP = ("z", "x", "c")
BF = jnp.bfloat16
F32 = jnp.float32


class Place:
    def __init__(self, sizes):
        self.ry, self.rx, self.z, self.x, self.c = (lax.axis_index(a) for a in REPLICA + FSDP)
        self.deep, self.wide, self.copies = sizes["z"], sizes["rx"], sizes["ry"] * sizes["rx"]
        self.half = self.deep // 2
        self.replica = self.ry * self.wide + self.rx
        self.xn = {"x": 1 - self.x}
        self.cn = {"c": 1 - self.c}
        self.zn = {"+": {"z": self.at(1)}, "-": {"z": self.at(-1)}}

    def at(self, offset):
        return lax.rem(self.z + offset + self.deep, self.deep)

    def block(self, z, x, c):
        return (z * 2 + x) * 2 + c

    def other(self, offset):
        return lax.rem(self.replica + offset, self.copies)

    def peer(self, replica):
        return {"ry": replica // self.wide, "rx": lax.rem(replica, self.wide)}


class Wires:
    def __init__(self, send_sems, recv_sems, anyone):
        self.send_sems, self.recv_sems, self.anyone = send_sems, recv_sems, anyone
        self.keys, self.started = {}, []

    def key(self, key):
        return self.recv_sems.at[self.keys.setdefault(key, len(self.keys))]

    def send(self, src, dst, to, key):
        copy = pltpu.make_async_remote_copy(
            src_ref=src,
            dst_ref=dst,
            send_sem=self.send_sems.at[len(self.started)],
            recv_sem=self.key(key),
            device_id=to,
            device_id_type=MESH,
        )
        copy.start()
        self.started.append(copy)

    def wait(self, ref, key):
        pltpu.make_async_remote_copy(
            src_ref=ref,
            dst_ref=ref,
            send_sem=self.send_sems.at[0],
            recv_sem=self.key(key),
            device_id=self.anyone,
            device_id_type=MESH,
        ).wait_recv()

    def drain(self):
        for copy in self.started:
            copy.wait_send()


def greet(p):
    barrier = pltpu.get_barrier_semaphore()
    friends = [p.xn, p.cn, p.zn["+"], p.zn["-"]]
    friends += [p.peer(p.other(o)) for o in range(1, p.copies)]
    for friend in friends:
        pl.semaphore_signal(barrier, inc=1, device_id=friend, device_id_type=MESH)
    pl.semaphore_wait(barrier, len(friends))


def hops_of(half):
    reach = {}
    for name in ("a1", "o"):
        reach["+", name], reach["-", name] = half, half - 1
    for name in ("a2", "t"):
        reach["+", name], reach["-", name] = half - 1, half
    return reach


NAMES = ("a1", "a2", "o", "t")


def gather(w, tag, full, p):
    q = full.shape[-1] // 4
    cols = {"a1": pl.ds(0, q), "a2": pl.ds(q, q), "o": pl.ds(2 * q, 2 * q), "t": pl.ds(2 * q, 2 * q)}
    reach = hops_of(p.half)
    whole = pl.ds(0, 4 * q)
    steps, arrivals = [], []

    def piece(z, x, c, name):
        return full.at[p.block(z, x, c), :, whole if name == "all" else cols[name]]

    def put(z, x, name, to, key):
        ref = piece(z, x, p.c, name)
        w.send(ref, ref, to, key)

    def share(z, x, name, key):
        put(z, x, name, p.cn, (tag, "c") + key)
        arrivals.append((z, x, name, (tag, "c") + key))

    def own():
        put(p.z, p.x, "o", p.xn, (tag, "xb"))
        for name in ("a1", "a2", "o"):
            for way in "+-":
                put(p.z, p.x, name, p.zn[way], (tag, way, 1, name))
        for name in ("a1", "a2"):
            put(p.z, p.x, name, p.xn, (tag, "xa", "+", 0, name))
        share(p.z, p.x, "all", ("own",))

    def crossed():
        w.wait(piece(p.z, 1 - p.x, p.c, "t"), (tag, "xb"))
        for way in "+-":
            put(p.z, 1 - p.x, "t", p.zn[way], (tag, way, 1, "t"))
        share(p.z, 1 - p.x, "t", ("xb",))

    def from_x(way, s, name):
        z = p.at(-s if way == "+" else s)
        w.wait(piece(z, 1 - p.x, p.c, name), (tag, "xa", way, s, name))
        share(z, 1 - p.x, name, ("xa", way, s, name))

    def from_z(way, s, name):
        z = p.at(-s if way == "+" else s)
        x = 1 - p.x if name == "t" else p.x
        w.wait(piece(z, x, p.c, name), (tag, way, s, name))
        if s < reach[way, name]:
            put(z, x, name, p.zn[way], (tag, way, s + 1, name))
        if name in ("a1", "a2"):
            put(z, x, name, p.xn, (tag, "xa", way, s, name))
        share(z, x, name, (way, s, name))

    def last():
        for z, x, name, key in list(arrivals):
            w.wait(piece(z, x, 1 - p.c, name), key)

    steps += [own, crossed]
    steps += [functools.partial(from_x, "+", 0, name) for name in ("a1", "a2")]
    for s in range(1, p.half + 1):
        for name in NAMES:
            for way in "+-":
                if s <= reach[way, name]:
                    steps.append(functools.partial(from_z, way, s, name))
        for name in ("a1", "a2"):
            for way in "+-":
                if 1 <= s - 1 <= reach[way, name]:
                    steps.append(functools.partial(from_x, way, s - 1, name))
    for name in ("a1", "a2"):
        for way in "+-":
            if p.half <= reach[way, name]:
                steps.append(functools.partial(from_x, way, p.half, name))
    steps.append(last)
    return steps


def exchange(w, tag, src, spread, chosen, dst, pick, p):
    width = src.shape[-1] // p.copies

    def chunk(k):
        return pl.ds(pl.multiple_of(k * width, width), width)

    def out():
        for o in range(1, p.copies):
            k = p.other(o)
            w.send(src.at[:, chunk(k)], spread.at[p.replica], p.peer(k), (tag, "out", o))
        spread[p.replica] = src[:, chunk(p.replica)]

    def through():
        for o in range(1, p.copies):
            w.wait(spread.at[p.other(p.copies - o)], (tag, "out", o))
        for o in range(1, p.copies):
            r = p.other(o)
            chosen[o] = spread[pick(r)]
            w.send(chosen.at[o], dst.at[:, chunk(p.replica)], p.peer(r), (tag, "back", o))
        dst[:, chunk(p.replica)] = spread[pick(p.replica)]

    def back():
        for o in range(1, p.copies):
            w.wait(dst.at[:, chunk(p.other(p.copies - o))], (tag, "back", o))

    return [out, through, back]


def scatter(w, tag, part, got_c, put_x, got_x, put_z, got_z, put_b, got_b, p, finish):
    q = part.shape[-1] // 4
    a = pl.ds(0, 2 * q)
    cols = {"a1": pl.ds(0, q), "a2": pl.ds(q, q), "o": pl.ds(2 * q, 2 * q), "t": pl.ds(2 * q, 2 * q)}
    slot = {"a1": pl.ds(0, q), "a2": pl.ds(q, q), "o": pl.ds(2 * q, 2 * q), "t": pl.ds(4 * q, 2 * q)}
    reach = hops_of(p.half)
    index = {"+": 0, "-": 1}
    steps = []
    seen = set()

    def pair(z, x, where):
        return part[z, x, p.c, :, where].astype(F32) + got_c[z, x, :, where].astype(F32)

    def offsets(d):
        return (0,) if d == 0 else ((d,) if d == p.half else (d, -d))

    def halves():
        for d in range(p.half, -1, -1):
            for o in offsets(d):
                z = p.at(o)
                w.send(part.at[z, :, 1 - p.c], got_c.at[z], p.cn, (tag, "c", o))

    def cross(o):
        z = p.at(o)
        w.wait(got_c.at[z], (tag, "c", o))
        put_x[z] = pair(z, 1 - p.x, a).astype(BF)
        w.send(put_x.at[z], got_x.at[z], p.xn, (tag, "x", o))

    def value(z, name, where):
        x = 1 - p.x if name == "t" else p.x
        total = pair(z, x, where)
        if name in ("a1", "a2"):
            total += got_x[z, :, where].astype(F32)
        return total

    def arrived(o, name):
        if name in ("a1", "a2") and o not in seen:
            seen.add(o)
            w.wait(got_x.at[p.at(o)], (tag, "x", o))

    def came(way, d, name):
        ref = got_z.at[index[way], d - 1, :, slot[name]]
        w.wait(ref, (tag, way, d, name))
        return ref[...].astype(F32)

    def onward(way, d, name):
        o = d if way == "+" else (p.half if d == p.half else -d)
        z = p.at(o)
        arrived(o, name)
        total = value(z, name, cols[name])
        if d < reach[way, name]:
            total += came(way, d + 1, name)
        ref = put_z.at[index[way], d - 1, :, slot[name]]
        ref[...] = total.astype(BF)
        w.send(ref, got_z.at[index[way], d - 1, :, slot[name]], p.zn[way], (tag, way, d, name))

    def ended(name):
        arrived(0, name)
        total = value(p.z, name, cols[name])
        for way in "+-":
            if 1 <= reach[way, name]:
                total += came(way, 1, name)
        return total

    def hand():
        put_b[...] = ended("t").astype(BF)
        w.send(put_b, got_b, p.xn, (tag, "b"))
        finish(cols["a1"], ended("a1"))
        finish(cols["a2"], ended("a2"))

    def last():
        total = ended("o")
        w.wait(got_b, (tag, "b"))
        finish(cols["o"], total + got_b[...].astype(F32))

    steps.append(halves)
    for d in range(p.half, 0, -1):
        steps += [functools.partial(cross, o) for o in offsets(d)]
        for name in ("t", "o", "a1", "a2"):
            for way in "+-":
                if d <= reach[way, name]:
                    steps.append(functools.partial(onward, way, d, name))
    steps += [functools.partial(cross, 0), hand, last]
    return steps


def token_kernel(sizes, partner, tokens, full, spread, chosen, load_sem, send_sems, recv_sems):
    p = Place(sizes)
    me = p.block(p.z, p.x, p.c)
    load = pltpu.make_async_copy(tokens, full.at[0, me], load_sem)
    load.start()
    greet(p)
    load.wait()
    w = Wires(send_sems, recv_sems, p.cn)

    def pick(replica):
        found = jnp.int32(0)
        for r in range(p.copies):
            found = jnp.maximum(found, jnp.where(partner[r] == replica, jnp.int32(r), jnp.int32(0)))
        return found

    out, through, back = exchange(w, "e", full.at[0, me], spread, chosen, full.at[1, me], pick, p)
    own, taught = gather(w, "s", full.at[0], p), gather(w, "t", full.at[1], p)
    out()
    own[0]()
    own[1]()
    through()
    for step in own[2:12]:
        step()
    back()
    taught[0]()
    for step in own[12:-1]:
        step()
    for step in taught[1:]:
        step()
    own[-1]()
    w.drain()


def result_kernel(
    sizes, scale, partner, part, full, got_c, put_x, got_x, put_z, got_z, put_b, got_b,
    mine, taught, teacher, spread, chosen, send_sems, recv_sems,
):
    p = Place(sizes)
    me = p.block(p.z, p.x, p.c)
    greet(p)
    w = Wires(send_sems, recv_sems, p.cn)

    def keep_taught(where, value):
        taught[:, where] = value.astype(BF)

    def keep_mine(where, value):
        mine[:, where] = value

    runs = [
        scatter(w, tag, *(r.at[k] for r in (part, got_c, put_x, got_x, put_z, got_z, put_b, got_b)), p, keep)
        for tag, k, keep in (("t", 1, keep_taught), ("s", 0, keep_mine))
    ]
    out, through, back = exchange(w, "e", taught, spread, chosen, teacher, lambda r: partner[r], p)
    runs[0][0]()
    runs[1][0]()
    for step in runs[0][1:]:
        step()
    out()
    middle = len(runs[1]) // 3
    for step in runs[1][1:middle]:
        step()
    through()
    for step in runs[1][middle:]:
        step()
    back()
    full[me] = ((mine[...] - teacher[...].astype(F32)) * scale).astype(BF)
    for step in gather(w, "g", full, p):
        step()
    w.drain()


def vmem():
    return pl.BlockSpec(memory_space=pltpu.VMEM)


def params(number):
    return pltpu.CompilerParams(
        collective_id=number, has_side_effects=True, vmem_limit_bytes=60 * 1024 * 1024
    )


def fetch_tokens(sizes, partner, tokens):
    rows, width = tokens.shape
    members, copies = sizes["z"] * 4, sizes["ry"] * sizes["rx"]
    return pl.pallas_call(
        functools.partial(token_kernel, sizes),
        out_shape=jax.ShapeDtypeStruct((2, members, rows, width), BF),
        in_specs=[pl.BlockSpec(memory_space=pltpu.SMEM), pl.BlockSpec(memory_space=pl.ANY)],
        out_specs=vmem(),
        scratch_shapes=[
            pltpu.VMEM((copies, rows, width // copies), BF),
            pltpu.VMEM((copies, rows, width // copies), BF),
            pltpu.SemaphoreType.DMA,
            pltpu.SemaphoreType.DMA((256,)),
            pltpu.SemaphoreType.DMA((256,)),
        ],
        compiler_params=params(0),
        name="fetch_tokens",
    )(partner, tokens)


def cotangents(sizes, scale, partner, part):
    rows, width = part.shape[-2:]
    deep, members, copies = sizes["z"], sizes["z"] * 4, sizes["ry"] * sizes["rx"]
    half, q = deep // 2, width // 4
    return pl.pallas_call(
        functools.partial(result_kernel, sizes, scale),
        out_shape=jax.ShapeDtypeStruct((members, rows, width), BF),
        in_specs=[pl.BlockSpec(memory_space=pltpu.SMEM), vmem()],
        out_specs=vmem(),
        scratch_shapes=[
            pltpu.VMEM((2, deep, 2, rows, width), BF),
            pltpu.VMEM((2, deep, rows, 2 * q), BF),
            pltpu.VMEM((2, deep, rows, 2 * q), BF),
            pltpu.VMEM((2, 2, half, rows, 6 * q), BF),
            pltpu.VMEM((2, 2, half, rows, 6 * q), BF),
            pltpu.VMEM((2, rows, 2 * q), BF),
            pltpu.VMEM((2, rows, 2 * q), BF),
            pltpu.VMEM((rows, width), F32),
            pltpu.VMEM((rows, width), BF),
            pltpu.VMEM((rows, width), BF),
            pltpu.VMEM((copies, rows, width // copies), BF),
            pltpu.VMEM((copies, rows, width // copies), BF),
            pltpu.SemaphoreType.DMA((320,)),
            pltpu.SemaphoreType.DMA((320,)),
        ],
        compiler_params=params(1),
        name="cotangents",
    )(partner, part)


def contract(left, right, left_dim, right_dim):
    return lax.dot_general(
        left, right, (((left_dim,), (right_dim,)), ((), ())), preferred_element_type=F32
    )


def local(sizes, partner, tokens, w_gate, w_up, w_down):
    rows, width = tokens.shape[1:]
    members = sizes["z"] * 4
    count = rows * members
    scale = 1.0 / math.sqrt(count)
    full = fetch_tokens(sizes, partner, tokens[0])
    both = full.reshape(2 * count, width)
    gates = contract(w_gate[0], both, 1, 1)
    ups = contract(w_up[0], both, 1, 1)
    hiddens = (jax.nn.silu(gates) * ups).astype(BF)
    part = contract(hiddens, w_down[0], 0, 0).astype(BF)
    cot = cotangents(sizes, scale, partner, part.reshape(2, sizes["z"], 2, 2, rows, width))
    cot = cot.reshape(count, width)
    rows_all, hidden, pre_gate, pre_up = both[:count], hiddens[:, :count], gates[:, :count], ups[:, :count]
    grad_down = contract(hidden, cot, 1, 0).astype(BF)
    d_hidden = contract(w_down[0], cot, 1, 1)
    sigma = jax.nn.sigmoid(pre_gate)
    d_gate = (d_hidden * pre_up * sigma * (1.0 + pre_gate * (1.0 - sigma))).astype(BF)
    d_up = (d_hidden * pre_gate * sigma).astype(BF)
    grad_gate = contract(d_gate, rows_all, 1, 0).astype(BF)
    grad_up = contract(d_up, rows_all, 1, 0).astype(BF)
    return (grad_gate[None], grad_up[None], grad_down[None])


def solution(mesh):
    members, copies = mesh.shape["fsdp"], mesh.shape["replica"]
    sizes = {"ry": copies // 2, "rx": 2, "z": members // 4, "x": 2, "c": 2}
    split = Mesh(mesh.devices.reshape(tuple(sizes.values())), tuple(sizes))
    spec = P(REPLICA, FSDP, None)
    return jax.shard_map(
        functools.partial(local, sizes),
        mesh=split,
        in_specs=(P(), spec, spec, spec, spec),
        out_specs=(spec, spec, spec),
        check_vma=False,
    )
```

```python
import functools
import math

import jax
import jax.numpy as jnp
from jax import lax
from jax.experimental import pallas as pl
from jax.experimental.pallas import tpu as pltpu
from jax.sharding import Mesh
from jax.sharding import PartitionSpec as P

MESH = pl.DeviceIdType.MESH
REPLICA = ("ry", "rx")
FSDP = ("z", "x", "c")
BF = jnp.bfloat16
NS, NR, LEAD = 24, 232, 22
F32 = jnp.float32


class Place:
    def __init__(self, sizes):
        self.ry, self.rx, self.z, self.x, self.c = (lax.axis_index(a) for a in REPLICA + FSDP)
        self.deep, self.wide, self.copies = sizes["z"], sizes["rx"], sizes["ry"] * sizes["rx"]
        self.half = self.deep // 2
        self.replica = self.ry * self.wide + self.rx
        self.xn = {"x": 1 - self.x}
        self.cn = {"c": 1 - self.c}
        self.zn = {"+": {"z": self.at(1)}, "-": {"z": self.at(-1)}}

    def at(self, offset):
        return lax.rem(self.z + offset + self.deep, self.deep)

    def block(self, z, x, c):
        return (z * 2 + x) * 2 + c

    def other(self, offset):
        return lax.rem(self.replica + offset, self.copies)

    def peer(self, replica):
        return {"ry": replica // self.wide, "rx": lax.rem(replica, self.wide)}


class Wires:
    def __init__(self, send_sems, recv_sems, anyone):
        self.send_sems, self.recv_sems, self.anyone = send_sems, recv_sems, anyone
        self.keys, self.groups = {}, {}

    def key(self, key):
        return self.recv_sems.at[self.keys.setdefault(key, len(self.keys))]

    def send(self, src, dst, to, key, group):
        number, total = self.groups.setdefault(group, (len(self.groups), []))
        total.append(math.prod(src.shape))
        pltpu.make_async_remote_copy(
            src_ref=src,
            dst_ref=dst,
            send_sem=self.send_sems.at[number],
            recv_sem=self.key(key),
            device_id=to,
            device_id_type=MESH,
        ).start()

    def of(self, ref, semaphore):
        return pltpu.make_async_remote_copy(
            src_ref=ref,
            dst_ref=ref,
            send_sem=semaphore,
            recv_sem=semaphore,
            device_id=self.anyone,
            device_id_type=MESH,
        )

    def wait(self, ref, key):
        self.of(ref, self.key(key)).wait_recv()

    def drain(self, sized):
        for number, total in self.groups.values():
            self.of(sized(sum(total)), self.send_sems.at[number]).wait_send()


def greet(p):
    barrier = pltpu.get_barrier_semaphore()
    friends = [p.xn, p.cn, p.zn["+"], p.zn["-"]]
    friends += [p.peer(p.other(o)) for o in range(1, p.copies)]
    for friend in friends:
        pl.semaphore_signal(barrier, inc=1, device_id=friend, device_id_type=MESH)
    pl.semaphore_wait(barrier, len(friends))


def hops_of(half):
    reach = {}
    for name in ("a1", "o"):
        reach["+", name], reach["-", name] = half, half - 1
    for name in ("a2", "t"):
        reach["+", name], reach["-", name] = half - 1, half
    return reach


NAMES = ("a1", "a2", "o", "t")


def gather(w, tag, full, p):
    q = full.shape[-1] // 4
    cols = {"a1": pl.ds(0, q), "a2": pl.ds(q, q), "o": pl.ds(2 * q, 2 * q), "t": pl.ds(2 * q, 2 * q)}
    reach = hops_of(p.half)
    whole = pl.ds(0, 4 * q)
    steps = []

    def piece(z, x, c, name):
        return full.at[p.block(z, x, c), :, whole if name == "all" else cols[name]]

    def put(z, x, name, to, key):
        ref = piece(z, x, p.c, name)
        w.send(ref, ref, to, key, (tag, "z" + key[1] if to is p.zn["+"] or to is p.zn["-"] else "x"))

    def share(z, x, name):
        ref = piece(z, x, p.c, name)
        w.send(ref, ref, p.cn, (tag, "c"), (tag, "c"))

    def own():
        put(p.z, p.x, "o", p.xn, (tag, "xb"))
        for name in ("a1", "a2", "o"):
            for way in "+-":
                put(p.z, p.x, name, p.zn[way], (tag, way, 1, name))
        for name in ("a1", "a2"):
            put(p.z, p.x, name, p.xn, (tag, "xa", "+", 0, name))
        share(p.z, p.x, "all")

    def crossed():
        w.wait(piece(p.z, 1 - p.x, p.c, "t"), (tag, "xb"))
        for way in "+-":
            put(p.z, 1 - p.x, "t", p.zn[way], (tag, way, 1, "t"))
        share(p.z, 1 - p.x, "t")

    def from_x(way, s, name):
        z = p.at(-s if way == "+" else s)
        w.wait(piece(z, 1 - p.x, p.c, name), (tag, "xa", way, s, name))
        share(z, 1 - p.x, name)

    def from_z(way, s, name):
        z = p.at(-s if way == "+" else s)
        x = 1 - p.x if name == "t" else p.x
        w.wait(piece(z, x, p.c, name), (tag, way, s, name))
        if s < reach[way, name]:
            put(z, x, name, p.zn[way], (tag, way, s + 1, name))
        if name in ("a1", "a2"):
            put(z, x, name, p.xn, (tag, "xa", way, s, name))
        share(z, x, name)

    def last():
        w.wait(full.at[pl.ds(0, 2 * p.deep)], (tag, "c"))

    steps += [own, crossed]
    steps += [functools.partial(from_x, "+", 0, name) for name in ("a1", "a2")]
    for s in range(1, p.half + 1):
        for name in NAMES:
            for way in "+-":
                if s <= reach[way, name]:
                    steps.append(functools.partial(from_z, way, s, name))
        for name in ("a1", "a2"):
            for way in "+-":
                if 1 <= s - 1 <= reach[way, name]:
                    steps.append(functools.partial(from_x, way, s - 1, name))
    for name in ("a1", "a2"):
        for way in "+-":
            if p.half <= reach[way, name]:
                steps.append(functools.partial(from_x, way, p.half, name))
    steps.append(last)
    return steps


def exchange(w, tag, src, spread, chosen, dst, pick, p):
    width = src.shape[-1] // p.copies

    def chunk(k):
        return pl.ds(pl.multiple_of(k * width, width), width)

    def out():
        for o in range(1, p.copies):
            k = p.other(o)
            w.send(src.at[:, chunk(k)], spread.at[p.replica], p.peer(k), (tag, "out"), (tag, "out"))
        spread[p.replica] = src[:, chunk(p.replica)]

    def through():
        w.wait(spread.at[pl.ds(0, p.copies - 1)], (tag, "out"))
        for o in range(1, p.copies):
            r = p.other(o)
            chosen[o] = spread[pick(r)]
            w.send(chosen.at[o], dst.at[:, chunk(p.replica)], p.peer(r), (tag, "back"), (tag, "back"))
        dst[:, chunk(p.replica)] = spread[pick(p.replica)]

    def back():
        w.wait(dst.at[:, pl.ds(0, (p.copies - 1) * width)], (tag, "back"))

    return [out, through, back]


def scatter(w, tag, part, got_c, put_x, got_x, put_z, got_z, put_b, got_b, p, finish):
    q = part.shape[-1] // 4
    a = pl.ds(0, 2 * q)
    cols = {"a1": pl.ds(0, q), "a2": pl.ds(q, q), "o": pl.ds(2 * q, 2 * q), "t": pl.ds(2 * q, 2 * q)}
    slot = {"a1": pl.ds(0, q), "a2": pl.ds(q, q), "o": pl.ds(2 * q, 2 * q), "t": pl.ds(4 * q, 2 * q)}
    reach = hops_of(p.half)
    index = {"+": 0, "-": 1}
    steps = []
    seen = set()

    def pair(z, x, where):
        return part[z, x, p.c, :, where].astype(F32) + got_c[z, x, :, where].astype(F32)

    def offsets(d):
        return (0,) if d == 0 else ((d,) if d == p.half else (d, -d))

    def halves():
        for d in range(p.half, -1, -1):
            for o in offsets(d):
                z = p.at(o)
                w.send(part.at[z, :, 1 - p.c], got_c.at[z], p.cn, (tag, "c", o), (tag, "c"))

    def cross(o):
        z = p.at(o)
        w.wait(got_c.at[z], (tag, "c", o))
        put_x[z] = pair(z, 1 - p.x, a).astype(BF)
        w.send(put_x.at[z], got_x.at[z], p.xn, (tag, "x", o), (tag, "x"))

    def value(z, name, where):
        x = 1 - p.x if name == "t" else p.x
        total = pair(z, x, where)
        if name in ("a1", "a2"):
            total += got_x[z, :, where].astype(F32)
        return total

    def arrived(o, name):
        if name in ("a1", "a2") and o not in seen:
            seen.add(o)
            w.wait(got_x.at[p.at(o)], (tag, "x", o))

    def came(way, d, name):
        ref = got_z.at[index[way], d - 1, :, slot[name]]
        w.wait(ref, (tag, way, d, name))
        return ref[...].astype(F32)

    def onward(way, d, name):
        o = d if way == "+" else (p.half if d == p.half else -d)
        z = p.at(o)
        arrived(o, name)
        total = value(z, name, cols[name])
        if d < reach[way, name]:
            total += came(way, d + 1, name)
        ref = put_z.at[index[way], d - 1, :, slot[name]]
        ref[...] = total.astype(BF)
        w.send(ref, got_z.at[index[way], d - 1, :, slot[name]], p.zn[way], (tag, way, d, name), (tag, "z" + way))

    def ended(name):
        arrived(0, name)
        total = value(p.z, name, cols[name])
        for way in "+-":
            if 1 <= reach[way, name]:
                total += came(way, 1, name)
        return total

    def hand():
        put_b[...] = ended("t").astype(BF)
        w.send(put_b, got_b, p.xn, (tag, "b"), (tag, "x"))
        finish(cols["a1"], ended("a1"))
        finish(cols["a2"], ended("a2"))

    def last():
        total = ended("o")
        w.wait(got_b, (tag, "b"))
        finish(cols["o"], total + got_b[...].astype(F32))

    def outward(d, names, fresh):
        return [
            functools.partial(onward, way, d, name)
            for name in names
            for way in "+-"
            if (d == reach[way, name] if fresh else d < reach[way, name])
        ]

    def crosses(d):
        return [functools.partial(cross, o) for o in offsets(d)] if d >= 0 else []

    top = p.half
    steps += [halves] + crosses(top) + outward(top, ("o", "t"), True)
    steps += crosses(top - 1) + outward(top - 1, ("o", "t"), True) + crosses(top - 2)
    steps += outward(top, ("a1", "a2"), True) + outward(top - 1, ("a1", "a2"), True)
    for d in range(top - 1, 0, -1):
        steps += outward(d, ("a1", "a2"), False) + crosses(d - 2) + outward(d, ("o", "t"), False)
    steps += [hand, last]
    return steps


def contract(left, right, left_dim, right_dim):
    return lax.dot_general(
        left, right, (((left_dim,), (right_dim,)), ((), ())), preferred_element_type=F32
    )


def mixed(steps, work):
    done = 0
    for k, step in enumerate(steps):
        step()
        while done < len(work) * (k + 1) // len(steps):
            work[done]()
            done += 1
    for piece in work[done:]:
        piece()


def forward(rows, pre, hidden, part, both_t, w_down):
    members, high, width = rows.shape
    q, units, lane = width // 4, hidden.shape[1], pre.shape[1] // 2
    count = members * high

    def grow(k):
        where = pl.ds(k * q, q)
        product = contract(rows[:, :, where].reshape(count, q), both_t[where, :], 1, 0)
        pre[...] = product if k == 0 else pre[...] + product

    def activate():
        gate = pre[:, pl.ds(0, units)]
        hidden[...] = (gate * jax.nn.sigmoid(gate) * pre[:, pl.ds(lane, units)]).astype(BF)

    def lower(k):
        where = pl.ds(k * q, q)
        product = contract(hidden[...], w_down[:, where], 1, 0).astype(BF)
        part[..., where] = product.reshape(part.shape[:-1] + (q,))

    work = [functools.partial(grow, k) for k in range(4)]
    return work + [activate] + [functools.partial(lower, k) for k in range(4)]


def kernel(sizes, scale, *refs):
    (
        partner, tokens, gate_in, up_in, down_in,
        rows_out, cot_out, hidden, d_gate, d_up,
        full, cot, w_gate, w_up, w_down, both_t, down_t, pre, far_pre, far_hidden,
        part, got_c, put_x, got_x, put_z, got_z, put_b, got_b,
        mine, taught, teacher, spread, chosen, spread_back, chosen_back, load_sems, send_sems, recv_sems,
    ) = refs
    p = Place(sizes)
    me = p.block(p.z, p.x, p.c)
    q = full.shape[-1] // 4
    load = pltpu.make_async_copy(tokens, full.at[me], load_sems.at[0])
    load.start()
    weights = [
        pltpu.make_async_copy(src, dst, load_sems.at[1 + k])
        for k, (src, dst) in enumerate(((gate_in, w_gate), (up_in, w_up), (down_in, w_down)))
    ]
    for copy in weights:
        copy.start()
    greet(p)
    load.wait()
    w = Wires(send_sems, recv_sems, p.cn)

    def taught_by(replica):
        found = jnp.int32(0)
        for r in range(p.copies):
            found = jnp.maximum(found, jnp.where(partner[r] == replica, jnp.int32(r), jnp.int32(0)))
        return found

    def keep_taught(where, value):
        taught[:, where] = value.astype(BF)

    def keep_mine(where, value):
        mine[:, where] = value

    rows_near, rows_far = (full.at[pl.ds(k * 4 * p.deep, 4 * p.deep)] for k in range(2))
    out, through, back = exchange(
        w, "e", rows_near.at[me], spread, chosen, rows_far.at[me], taught_by, p
    )
    near, far = gather(w, "s", rows_near, p), gather(w, "t", rows_far, p)
    near_work = forward(rows_near, pre, hidden, part.at[0], both_t, w_down)
    far_work = forward(rows_far, far_pre, far_hidden, part.at[1], both_t, w_down)
    near_sum, far_sum = (
        scatter(w, tag, *(r.at[k] for r in (part, got_c, put_x, got_x, put_z, got_z, put_b, got_b)), p, keep)
        for tag, k, keep in (("a", 0, keep_mine), ("b", 1, keep_taught))
    )
    back_out, back_through, back_back = exchange(
        w, "f", taught, spread_back, chosen_back, teacher, lambda r: partner[r], p
    )

    units, lane = hidden.shape[1], pre.shape[1] // 2

    def turn(src, dst, start, k):
        where = pl.ds(k * q, q)
        dst[where, pl.ds(start, units)] = src[:, where].T
        if dst is both_t and lane > units:
            dst[where, pl.ds(start + units, lane - units)] = jnp.zeros((q, lane - units), BF)

    turns = [
        functools.partial(turn, src, dst, start, k)
        for src, dst, start in ((w_gate, both_t, 0), (w_up, both_t, lane), (w_down, down_t, 0))
        for k in range(4)
    ]
    near[0]()
    out()
    for copy in weights:
        copy.wait()
    mixed(near[1:12], turns)
    through()
    mixed(near[12:24], [])
    back()
    far[0]()
    mixed(near[24:34], [])
    mixed(far[1:4], [])
    mixed(near[34:-1], far[4:12])
    near[-1]()
    keep_rows = pltpu.make_async_copy(rows_near, rows_out, load_sems.at[4])
    keep_rows.start()
    mixed(far[12:], near_work)
    near_sum[0]()
    mixed(far_work, near_sum[1:9])
    far_sum[0]()
    mixed(far_sum[1:9], [])
    mixed(far_sum[9:], near_sum[9:LEAD])
    back_out()
    mixed(near_sum[LEAD:-6], [])
    back_through()
    mixed(near_sum[-6:], [])
    back_back()
    cot[me] = ((mine[...] - teacher[...].astype(F32)) * scale).astype(BF)
    mixed(gather(w, "g", cot, p), [])
    keep_cot = pltpu.make_async_copy(cot, cot_out, load_sems.at[5])
    keep_cot.start()
    count = pre.shape[0]

    def pull(k):
        where = pl.ds(k * q, q)
        product = contract(cot[:, :, where].reshape(count, q), down_t[where, :], 1, 0)
        here = pl.ds(0, units)
        far_pre[:, here] = product if k == 0 else far_pre[:, here] + product

    for k in range(4):
        pull(k)
    gate, up, d_hidden = pre[:, pl.ds(0, units)], pre[:, pl.ds(lane, units)], far_pre[:, pl.ds(0, units)]
    sigma = jax.nn.sigmoid(gate)
    d_gate[...] = (d_hidden * up * sigma * (1.0 + gate * (1.0 - sigma))).astype(BF)
    d_up[...] = (d_hidden * gate * sigma).astype(BF)
    keep_cot.wait()

    def sized(elements):
        unit = full.shape[1] * q
        if elements % unit:
            return chosen.at[pl.ds(0, p.copies - 1)]
        return full.at[pl.ds(0, elements // unit), :, pl.ds(0, q)]

    keep_rows.wait()
    w.drain(sized)


def fused(sizes, scale, partner, tokens, w_gate, w_up, w_down):
    rows, width = tokens.shape
    units = w_gate.shape[0]
    lane = pl.cdiv(units, 128) * 128
    deep, members, copies = sizes["z"], sizes["z"] * 4, sizes["ry"] * sizes["rx"]
    half, q, count = deep // 2, width // 4, rows * members
    anywhere, vmem = pl.BlockSpec(memory_space=pl.ANY), pl.BlockSpec(memory_space=pltpu.VMEM)
    chunk = pltpu.VMEM((copies, rows, width // copies), BF)
    return pl.pallas_call(
        functools.partial(kernel, sizes, scale),
        out_shape=[
            jax.ShapeDtypeStruct((members, rows, width), BF),
            jax.ShapeDtypeStruct((members, rows, width), BF),
            jax.ShapeDtypeStruct((count, units), BF),
            jax.ShapeDtypeStruct((count, units), BF),
            jax.ShapeDtypeStruct((count, units), BF),
        ],
        in_specs=[pl.BlockSpec(memory_space=pltpu.SMEM)] + [anywhere] * 4,
        out_specs=[anywhere] * 2 + [vmem] * 3,
        scratch_shapes=[
            pltpu.VMEM((2 * members, rows, width), BF),
            pltpu.VMEM((members, rows, width), BF),
            pltpu.VMEM((units, width), BF),
            pltpu.VMEM((units, width), BF),
            pltpu.VMEM((units, width), BF),
            pltpu.VMEM((width, 2 * lane), BF),
            pltpu.VMEM((width, units), BF),
            pltpu.VMEM((count, 2 * lane), F32),
            pltpu.VMEM((count, 2 * lane), F32),
            pltpu.VMEM((count, units), BF),
            pltpu.VMEM((2, deep, 2, 2, rows, width), BF),
            pltpu.VMEM((2, deep, 2, rows, width), BF),
            pltpu.VMEM((2, deep, rows, 2 * q), BF),
            pltpu.VMEM((2, deep, rows, 2 * q), BF),
            pltpu.VMEM((2, 2, half, rows, 6 * q), BF),
            pltpu.VMEM((2, 2, half, rows, 6 * q), BF),
            pltpu.VMEM((2, rows, 2 * q), BF),
            pltpu.VMEM((2, rows, 2 * q), BF),
            pltpu.VMEM((rows, width), F32),
            pltpu.VMEM((rows, width), BF),
            pltpu.VMEM((rows, width), BF),
            chunk,
            chunk,
            chunk,
            chunk,
            pltpu.SemaphoreType.DMA((6,)),
            pltpu.SemaphoreType.DMA((NS,)),
            pltpu.SemaphoreType.DMA((NR,)),
        ],
        compiler_params=pltpu.CompilerParams(
            collective_id=0, has_side_effects=True, vmem_limit_bytes=62 * 1024 * 1024
        ),
        name="step",
    )(partner, tokens, w_gate, w_up, w_down)


def local(sizes, partner, tokens, w_gate, w_up, w_down):
    rows, width = tokens.shape[1:]
    count = rows * sizes["z"] * 4
    scale = 1.0 / math.sqrt(count)
    rows_all, cot, hidden, d_gate, d_up = fused(
        sizes, scale, partner, tokens[0], w_gate[0], w_up[0], w_down[0]
    )
    rows_all, cot = rows_all.reshape(count, width), cot.reshape(count, width)
    grad_down = contract(hidden, cot, 0, 0).astype(BF)
    grad_gate = contract(d_gate, rows_all, 0, 0).astype(BF)
    grad_up = contract(d_up, rows_all, 0, 0).astype(BF)
    return (grad_gate[None], grad_up[None], grad_down[None])


def solution(mesh):
    members, copies = mesh.shape["fsdp"], mesh.shape["replica"]
    sizes = {"ry": copies // 2, "rx": 2, "z": members // 4, "x": 2, "c": 2}
    split = Mesh(mesh.devices.reshape(tuple(sizes.values())), tuple(sizes))
    spec = P(REPLICA, FSDP, None)
    return jax.shard_map(
        functools.partial(local, sizes),
        mesh=split,
        in_specs=(P(), spec, spec, spec, spec),
        out_specs=(spec, spec, spec),
        check_vma=False,
    )
```

```python
import functools
import math

import jax
import jax.numpy as jnp
from jax import lax
from jax.experimental import pallas as pl
from jax.experimental.pallas import tpu as pltpu
from jax.sharding import Mesh
from jax.sharding import PartitionSpec as P

MESH = pl.DeviceIdType.MESH
REPLICA = ("ry", "rx")
FSDP = ("z", "x", "c")
BF = jnp.bfloat16
NS, NR, EARLY, LEAD, LATE, PARTS = 24, 232, 7, 21, 4, 2
F32 = jnp.float32


class Place:
    def __init__(self, sizes):
        self.ry, self.rx, self.z, self.x, self.c = (lax.axis_index(a) for a in REPLICA + FSDP)
        self.deep, self.wide, self.copies = sizes["z"], sizes["rx"], sizes["ry"] * sizes["rx"]
        self.half = self.deep // 2
        self.replica = self.ry * self.wide + self.rx
        self.xn = {"x": 1 - self.x}
        self.cn = {"c": 1 - self.c}
        self.zn = {"+": {"z": self.at(1)}, "-": {"z": self.at(-1)}}

    def at(self, offset):
        return lax.rem(self.z + offset + self.deep, self.deep)

    def block(self, z, x, c):
        return (z * 2 + x) * 2 + c

    def other(self, offset):
        return lax.rem(self.replica + offset, self.copies)

    def peer(self, replica):
        return {"ry": replica // self.wide, "rx": lax.rem(replica, self.wide)}


class Wires:
    def __init__(self, send_sems, recv_sems, anyone):
        self.send_sems, self.recv_sems, self.anyone = send_sems, recv_sems, anyone
        self.keys, self.groups = {}, {}

    def key(self, key):
        return self.recv_sems.at[self.keys.setdefault(key, len(self.keys))]

    def send(self, src, dst, to, key, group):
        number, total = self.groups.setdefault(group, (len(self.groups), []))
        total.append(math.prod(src.shape))
        pltpu.make_async_remote_copy(
            src_ref=src,
            dst_ref=dst,
            send_sem=self.send_sems.at[number],
            recv_sem=self.key(key),
            device_id=to,
            device_id_type=MESH,
        ).start()

    def of(self, ref, semaphore):
        return pltpu.make_async_remote_copy(
            src_ref=ref,
            dst_ref=ref,
            send_sem=semaphore,
            recv_sem=semaphore,
            device_id=self.anyone,
            device_id_type=MESH,
        )

    def wait(self, ref, key):
        self.of(ref, self.key(key)).wait_recv()

    def drain(self, sized):
        for number, total in self.groups.values():
            self.of(sized(sum(total)), self.send_sems.at[number]).wait_send()


def greet(p):
    barrier = pltpu.get_barrier_semaphore()
    friends = [p.xn, p.cn, p.zn["+"], p.zn["-"]]
    friends += [p.peer(p.other(o)) for o in range(1, p.copies)]
    for friend in friends:
        pl.semaphore_signal(barrier, inc=1, device_id=friend, device_id_type=MESH)
    pl.semaphore_wait(barrier, len(friends))


def hops_of(half):
    reach = {}
    for name in ("a1", "o"):
        reach["+", name], reach["-", name] = half, half - 1
    for name in ("a2", "t"):
        reach["+", name], reach["-", name] = half - 1, half
    return reach


NAMES = ("a1", "a2", "o", "t")


def gather(w, tag, full, p):
    q = full.shape[-1] // 4
    cols = {"a1": pl.ds(0, q), "a2": pl.ds(q, q), "o": pl.ds(2 * q, 2 * q), "t": pl.ds(2 * q, 2 * q)}
    reach = hops_of(p.half)
    whole = pl.ds(0, 4 * q)
    steps = []

    def piece(z, x, c, name):
        return full.at[p.block(z, x, c), :, whole if name == "all" else cols[name]]

    def put(z, x, name, to, key):
        ref = piece(z, x, p.c, name)
        w.send(ref, ref, to, key, (tag, "z" + key[1] if to is p.zn["+"] or to is p.zn["-"] else "x"))

    def share(z, x, name):
        ref = piece(z, x, p.c, name)
        w.send(ref, ref, p.cn, (tag, "c"), (tag, "c"))

    def own():
        put(p.z, p.x, "o", p.xn, (tag, "xb"))
        for name in ("a1", "a2", "o"):
            for way in "+-":
                put(p.z, p.x, name, p.zn[way], (tag, way, 1, name))
        for name in ("a1", "a2"):
            put(p.z, p.x, name, p.xn, (tag, "xa", "+", 0, name))
        share(p.z, p.x, "all")

    def crossed():
        w.wait(piece(p.z, 1 - p.x, p.c, "t"), (tag, "xb"))
        for way in "+-":
            put(p.z, 1 - p.x, "t", p.zn[way], (tag, way, 1, "t"))
        share(p.z, 1 - p.x, "t")

    def from_x(way, s, name):
        z = p.at(-s if way == "+" else s)
        w.wait(piece(z, 1 - p.x, p.c, name), (tag, "xa", way, s, name))
        share(z, 1 - p.x, name)

    def from_z(way, s, name):
        z = p.at(-s if way == "+" else s)
        x = 1 - p.x if name == "t" else p.x
        w.wait(piece(z, x, p.c, name), (tag, way, s, name))
        if s < reach[way, name]:
            put(z, x, name, p.zn[way], (tag, way, s + 1, name))
        if name in ("a1", "a2"):
            put(z, x, name, p.xn, (tag, "xa", way, s, name))
        share(z, x, name)

    def last():
        w.wait(full.at[pl.ds(0, 2 * p.deep)], (tag, "c"))

    steps += [own, crossed]
    steps += [functools.partial(from_x, "+", 0, name) for name in ("a1", "a2")]
    for s in range(1, p.half + 1):
        for name in NAMES:
            for way in "+-":
                if s <= reach[way, name]:
                    steps.append(functools.partial(from_z, way, s, name))
        for name in ("a1", "a2"):
            for way in "+-":
                if 1 <= s - 1 <= reach[way, name]:
                    steps.append(functools.partial(from_x, way, s - 1, name))
    for name in ("a1", "a2"):
        for way in "+-":
            if p.half <= reach[way, name]:
                steps.append(functools.partial(from_x, way, p.half, name))
    steps.append(last)
    return steps


def exchange(w, tag, src, spread, chosen, dst, pick, p):
    width = src.shape[-1] // p.copies

    def chunk(k):
        return pl.ds(pl.multiple_of(k * width, width), width)

    def out():
        for o in range(1, p.copies):
            k = p.other(o)
            w.send(src.at[:, chunk(k)], spread.at[p.replica], p.peer(k), (tag, "out"), (tag, "out"))
        spread[p.replica] = src[:, chunk(p.replica)]

    def through():
        w.wait(spread.at[pl.ds(0, p.copies - 1)], (tag, "out"))
        for o in range(1, p.copies):
            r = p.other(o)
            chosen[o] = spread[pick(r)]
            w.send(chosen.at[o], dst.at[:, chunk(p.replica)], p.peer(r), (tag, "back"), (tag, "back"))
        dst[:, chunk(p.replica)] = spread[pick(p.replica)]

    def back():
        w.wait(dst.at[:, pl.ds(0, (p.copies - 1) * width)], (tag, "back"))

    return [out, through, back]


def scatter(w, tag, part, got_c, put_x, got_x, put_z, got_z, put_b, got_b, p, finish):
    q = part.shape[-1] // 4
    a = pl.ds(0, 2 * q)
    cols = {"a1": pl.ds(0, q), "a2": pl.ds(q, q), "o": pl.ds(2 * q, 2 * q), "t": pl.ds(2 * q, 2 * q)}
    slot = {"a1": pl.ds(0, q), "a2": pl.ds(q, q), "o": pl.ds(2 * q, 2 * q), "t": pl.ds(4 * q, 2 * q)}
    reach = hops_of(p.half)
    index = {"+": 0, "-": 1}
    steps = []
    seen = set()

    def pair(z, x, where):
        return part[z, x, p.c, :, where].astype(F32) + got_c[z, x, :, where].astype(F32)

    def offsets(d):
        return (0,) if d == 0 else ((d,) if d == p.half else (d, -d))

    def halves():
        for d in range(p.half, -1, -1):
            for o in offsets(d):
                z = p.at(o)
                w.send(part.at[z, :, 1 - p.c], got_c.at[z], p.cn, (tag, "c", o), (tag, "c"))

    def cross(o):
        z = p.at(o)
        w.wait(got_c.at[z], (tag, "c", o))
        put_x[z] = pair(z, 1 - p.x, a).astype(BF)
        w.send(put_x.at[z], got_x.at[z], p.xn, (tag, "x", o), (tag, "x"))

    def value(z, name, where):
        x = 1 - p.x if name == "t" else p.x
        total = pair(z, x, where)
        if name in ("a1", "a2"):
            total += got_x[z, :, where].astype(F32)
        return total

    def arrived(o, name):
        if name in ("a1", "a2") and o not in seen:
            seen.add(o)
            w.wait(got_x.at[p.at(o)], (tag, "x", o))

    def came(way, d, name):
        ref = got_z.at[index[way], d - 1, :, slot[name]]
        w.wait(ref, (tag, way, d, name))
        return ref[...].astype(F32)

    def onward(way, d, name):
        o = d if way == "+" else (p.half if d == p.half else -d)
        z = p.at(o)
        arrived(o, name)
        total = value(z, name, cols[name])
        if d < reach[way, name]:
            total += came(way, d + 1, name)
        ref = put_z.at[index[way], d - 1, :, slot[name]]
        ref[...] = total.astype(BF)
        w.send(ref, got_z.at[index[way], d - 1, :, slot[name]], p.zn[way], (tag, way, d, name), (tag, "z" + way))

    def ended(name):
        arrived(0, name)
        total = value(p.z, name, cols[name])
        for way in "+-":
            if 1 <= reach[way, name]:
                total += came(way, 1, name)
        return total

    def hand():
        put_b[...] = ended("t").astype(BF)
        w.send(put_b, got_b, p.xn, (tag, "b"), (tag, "x"))
        finish(cols["a1"], ended("a1"))
        finish(cols["a2"], ended("a2"))

    def last():
        total = ended("o")
        w.wait(got_b, (tag, "b"))
        finish(cols["o"], total + got_b[...].astype(F32))

    def outward(d, names, fresh):
        return [
            functools.partial(onward, way, d, name)
            for name in names
            for way in "+-"
            if (d == reach[way, name] if fresh else d < reach[way, name])
        ]

    def crosses(d):
        return [functools.partial(cross, o) for o in offsets(d)] if d >= 0 else []

    top = p.half
    steps += [halves] + crosses(top) + outward(top, ("t", "o"), True)
    steps += crosses(top - 1) + outward(top - 1, ("t", "o"), True) + crosses(top - 2)
    steps += outward(top, ("a1", "a2"), True) + outward(top - 1, ("a1", "a2"), True)
    for d in range(top - 1, 0, -1):
        steps += outward(d, ("t", "a1", "a2"), False) + crosses(d - 2) + outward(d, ("o",), False)
    steps += [hand, last]
    return steps


def contract(left, right, left_dim, right_dim):
    return lax.dot_general(
        left, right, (((left_dim,), (right_dim,)), ((), ())), preferred_element_type=F32
    )


def mixed(steps, work):
    done = 0
    for k, step in enumerate(steps):
        step()
        while done < len(work) * (k + 1) // len(steps):
            work[done]()
            done += 1
    for piece in work[done:]:
        piece()


def forward(rows, pre, hidden, part, both_t, w_down):
    members, high, width = rows.shape
    q, units, lane = width // 4, hidden.shape[1], pre.shape[1] // 2
    count = members * high

    def grow(k):
        where = pl.ds(k * q, q)
        product = contract(rows[:, :, where].reshape(count, q), both_t[where, :], 1, 0)
        pre[...] = product if k == 0 else pre[...] + product

    def activate():
        gate = pre[:, pl.ds(0, units)]
        hidden[...] = (gate * jax.nn.sigmoid(gate) * pre[:, pl.ds(lane, units)]).astype(BF)

    def lower(k):
        where = pl.ds(k * q, q)
        product = contract(hidden[...], w_down[:, where], 1, 0).astype(BF)
        part[..., where] = product.reshape(part.shape[:-1] + (q,))

    work = [functools.partial(grow, k) for k in range(4)]
    return work + [activate] + [functools.partial(lower, k) for k in range(4)]


def kernel(sizes, scale, *refs):
    (
        partner, tokens, gate_in, up_in, down_in,
        rows_out, cot_out, hidden_t, d_both_t,
        full, cot, w_gate, w_up, w_down, both_t, pre, far_pre, hidden, far_hidden, slope_gate, slope_up, d_hidden,
        part, got_c, put_x, got_x, put_z, got_z, put_b, got_b,
        mine, taught, teacher, spread, chosen, spread_back, chosen_back, load_sems, send_sems, recv_sems,
    ) = refs
    p = Place(sizes)
    me = p.block(p.z, p.x, p.c)
    q = full.shape[-1] // 4
    load = pltpu.make_async_copy(tokens, full.at[me], load_sems.at[0])
    load.start()
    weights = [
        pltpu.make_async_copy(src, dst, load_sems.at[1 + k])
        for k, (src, dst) in enumerate(((gate_in, w_gate), (up_in, w_up), (down_in, w_down)))
    ]
    for copy in weights:
        copy.start()
    greet(p)
    load.wait()
    w = Wires(send_sems, recv_sems, p.cn)

    def taught_by(replica):
        found = jnp.int32(0)
        for r in range(p.copies):
            found = jnp.maximum(found, jnp.where(partner[r] == replica, jnp.int32(r), jnp.int32(0)))
        return found

    def keep_taught(where, value):
        taught[:, where] = value.astype(BF)

    def keep_mine(where, value):
        mine[:, where] = value

    rows_near, rows_far = (full.at[pl.ds(k * 4 * p.deep, 4 * p.deep)] for k in range(2))
    out, through, back = exchange(
        w, "e", rows_near.at[me], spread, chosen, rows_far.at[me], taught_by, p
    )
    near, far = gather(w, "s", rows_near, p), gather(w, "t", rows_far, p)
    near_work = forward(rows_near, pre, hidden, part.at[0], both_t, w_down)
    far_work = forward(rows_far, far_pre, far_hidden, part.at[1], both_t, w_down)
    near_sum, far_sum = (
        scatter(w, tag, *(r.at[k] for r in (part, got_c, put_x, got_x, put_z, got_z, put_b, got_b)), p, keep)
        for tag, k, keep in (("a", 0, keep_mine), ("b", 1, keep_taught))
    )
    back_out, back_through, back_back = exchange(
        w, "f", taught, spread_back, chosen_back, teacher, lambda r: partner[r], p
    )

    units, lane = hidden.shape[1], pre.shape[1] // 2

    def turn(src, dst, start, k):
        where = pl.ds(k * q, q)
        dst[where, pl.ds(start, units)] = src[:, where].T
        if lane > units:
            dst[where, pl.ds(start + units, lane - units)] = jnp.zeros((q, lane - units), BF)

    turns = [
        functools.partial(turn, src, dst, start, k)
        for src, dst, start in ((w_gate, both_t, 0), (w_up, both_t, lane))
        for k in range(4)
    ]
    near[0]()
    out()
    for copy in weights:
        copy.wait()
    mixed(turns, [])
    mixed(near[1:12], [])
    through()
    mixed(near[12:24], [])
    back()
    far[0]()
    mixed(near[24:34], [])
    mixed(far[1:4], [])
    mixed(near[34:-1], far[4:12])
    near[-1]()
    keep_rows = pltpu.make_async_copy(rows_near, rows_out, load_sems.at[4])
    keep_rows.start()
    mixed(far[12:], near_work)
    near_sum[0]()
    mixed(far_work, near_sum[1:EARLY])
    far_sum[0]()
    mixed(far_sum[1:9], [])
    mixed(far_sum[9:-2], near_sum[EARLY:LEAD])
    far_sum[-2]()
    mixed(near_sum[LEAD : LEAD + 3], [])
    far_sum[-1]()
    back_out()
    mixed(near_sum[LEAD + 3 : -LATE], [])
    back_through()
    mixed(near_sum[-LATE:], [])
    back_back()
    cot[me] = ((mine[...] - teacher[...].astype(F32)) * scale).astype(BF)
    count = pre.shape[0]

    def derive(k):
        here = pl.ds(k * 128, 128)
        gate, up = pre[here, pl.ds(0, units)], pre[here, pl.ds(lane, units)]
        sigma = jax.nn.sigmoid(gate)
        slope_gate[:, here] = (up * sigma * (1.0 + gate * (1.0 - sigma))).T
        slope_up[:, here] = (gate * sigma).T
        hidden_t[:, here] = hidden[here, :].T

    last = gather(w, "g", cot, p)
    last[0]()
    for k in range(count // 128):
        derive(k)
    mixed(last[1:], [])
    keep_cot = pltpu.make_async_copy(cot, cot_out, load_sems.at[5])
    keep_cot.start()
    for k in range(4):
        where = pl.ds(k * q, q)
        product = contract(w_down[:, where], cot[:, :, where].reshape(count, q), 1, 1)
        d_hidden[...] = product if k == 0 else d_hidden[...] + product
    d_both_t[pl.ds(0, units), :] = (d_hidden[...] * slope_gate[...]).astype(BF)
    d_both_t[pl.ds(units, units), :] = (d_hidden[...] * slope_up[...]).astype(BF)
    keep_cot.wait()

    def sized(elements):
        unit = full.shape[1] * q
        if elements % unit:
            return chosen.at[pl.ds(0, p.copies - 1)]
        return full.at[pl.ds(0, elements // unit), :, pl.ds(0, q)]

    keep_rows.wait()
    w.drain(sized)


def fused(sizes, scale, partner, tokens, w_gate, w_up, w_down):
    rows, width = tokens.shape
    units = w_gate.shape[0]
    lane = pl.cdiv(units, 128) * 128
    deep, members, copies = sizes["z"], sizes["z"] * 4, sizes["ry"] * sizes["rx"]
    half, q, count = deep // 2, width // 4, rows * members
    anywhere, vmem = pl.BlockSpec(memory_space=pl.ANY), pl.BlockSpec(memory_space=pltpu.VMEM)
    chunk = pltpu.VMEM((copies, rows, width // copies), BF)
    return pl.pallas_call(
        functools.partial(kernel, sizes, scale),
        out_shape=[
            jax.ShapeDtypeStruct((members, rows, width), BF),
            jax.ShapeDtypeStruct((members, rows, width), BF),
            jax.ShapeDtypeStruct((units, count), BF),
            jax.ShapeDtypeStruct((2 * units, count), BF),
        ],
        in_specs=[pl.BlockSpec(memory_space=pltpu.SMEM)] + [anywhere] * 4,
        out_specs=[anywhere] * 2 + [vmem] * 2,
        scratch_shapes=[
            pltpu.VMEM((2 * members, rows, width), BF),
            pltpu.VMEM((members, rows, width), BF),
            pltpu.VMEM((units, width), BF),
            pltpu.VMEM((units, width), BF),
            pltpu.VMEM((units, width), BF),
            pltpu.VMEM((width, 2 * lane), BF),
            pltpu.VMEM((count, 2 * lane), F32),
            pltpu.VMEM((count, 2 * lane), F32),
            pltpu.VMEM((count, units), BF),
            pltpu.VMEM((count, units), BF),
            pltpu.VMEM((units, count), F32),
            pltpu.VMEM((units, count), F32),
            pltpu.VMEM((units, count), F32),
            pltpu.VMEM((2, deep, 2, 2, rows, width), BF),
            pltpu.VMEM((2, deep, 2, rows, width), BF),
            pltpu.VMEM((2, deep, rows, 2 * q), BF),
            pltpu.VMEM((2, deep, rows, 2 * q), BF),
            pltpu.VMEM((2, 2, half, rows, 6 * q), BF),
            pltpu.VMEM((2, 2, half, rows, 6 * q), BF),
            pltpu.VMEM((2, rows, 2 * q), BF),
            pltpu.VMEM((2, rows, 2 * q), BF),
            pltpu.VMEM((rows, width), F32),
            pltpu.VMEM((rows, width), BF),
            pltpu.VMEM((rows, width), BF),
            chunk,
            chunk,
            chunk,
            chunk,
            pltpu.SemaphoreType.DMA((6,)),
            pltpu.SemaphoreType.DMA((NS,)),
            pltpu.SemaphoreType.DMA((NR,)),
        ],
        compiler_params=pltpu.CompilerParams(
            collective_id=0, has_side_effects=True, vmem_limit_bytes=62 * 1024 * 1024
        ),
        name="step",
    )(partner, tokens, w_gate, w_up, w_down)


def products_kernel(hidden_t, d_both_t, rows, cot, grad_gate, grad_up, grad_down):
    units = hidden_t.shape[0]
    both = contract(d_both_t[...], rows[...], 1, 0).astype(BF)
    grad_gate[...] = both[:units]
    grad_up[...] = both[units:]
    grad_down[...] = contract(hidden_t[...], cot[...], 1, 0).astype(BF)


def products(hidden_t, d_both_t, rows, cot):
    (units, count), width = hidden_t.shape, rows.shape[1]
    step = width // PARTS
    columns = pl.BlockSpec((count, step), lambda j: (0, j))
    return pl.pallas_call(
        products_kernel,
        grid=(PARTS,),
        out_shape=[jax.ShapeDtypeStruct((units, width), BF)] * 3,
        in_specs=[
            pl.BlockSpec((units, count), lambda j: (0, 0)),
            pl.BlockSpec((2 * units, count), lambda j: (0, 0)),
            columns,
            columns,
        ],
        out_specs=[pl.BlockSpec((units, step), lambda j: (0, j))] * 3,
        compiler_params=pltpu.CompilerParams(dimension_semantics=("arbitrary",)),
        name="products",
    )(hidden_t, d_both_t, rows, cot)


def local(sizes, partner, tokens, w_gate, w_up, w_down):
    rows, width = tokens.shape[1:]
    count = rows * sizes["z"] * 4
    scale = 1.0 / math.sqrt(count)
    rows_all, cot, hidden_t, d_both_t = fused(
        sizes, scale, partner, tokens[0], w_gate[0], w_up[0], w_down[0]
    )
    grads = products(hidden_t, d_both_t, rows_all.reshape(count, width), cot.reshape(count, width))
    return tuple(grad[None] for grad in grads)


def solution(mesh):
    members, copies = mesh.shape["fsdp"], mesh.shape["replica"]
    sizes = {"ry": copies // 2, "rx": 2, "z": members // 4, "x": 2, "c": 2}
    split = Mesh(mesh.devices.reshape(tuple(sizes.values())), tuple(sizes))
    spec = P(REPLICA, FSDP, None)
    return jax.shard_map(
        functools.partial(local, sizes),
        mesh=split,
        in_specs=(P(), spec, spec, spec, spec),
        out_specs=(spec, spec, spec),
        check_vma=False,
    )
```

```python
import functools
import math

import jax
import jax.numpy as jnp
from jax import lax
from jax.experimental import pallas as pl
from jax.experimental.pallas import tpu as pltpu
from jax.sharding import Mesh
from jax.sharding import PartitionSpec as P

MESH = pl.DeviceIdType.MESH
REPLICA = ("ry", "rx")
FSDP = ("z", "x", "c")
BF = jnp.bfloat16
NS, NR, EARLY, LEAD, LATE, PARTS = 24, 232, 7, 19, 4, 2
F32 = jnp.float32


class Place:
    def __init__(self, sizes):
        self.ry, self.rx, self.z, self.x, self.c = (lax.axis_index(a) for a in REPLICA + FSDP)
        self.deep, self.wide, self.copies = sizes["z"], sizes["rx"], sizes["ry"] * sizes["rx"]
        self.half = self.deep // 2
        self.replica = self.ry * self.wide + self.rx
        self.xn = {"x": 1 - self.x}
        self.cn = {"c": 1 - self.c}
        self.zn = {"+": {"z": self.at(1)}, "-": {"z": self.at(-1)}}

    def at(self, offset):
        return lax.rem(self.z + offset + self.deep, self.deep)

    def block(self, z, x, c):
        return (z * 2 + x) * 2 + c

    def other(self, offset):
        return lax.rem(self.replica + offset, self.copies)

    def peer(self, replica):
        return {"ry": replica // self.wide, "rx": lax.rem(replica, self.wide)}


class Wires:
    def __init__(self, send_sems, recv_sems, anyone):
        self.send_sems, self.recv_sems, self.anyone = send_sems, recv_sems, anyone
        self.keys, self.groups = {}, {}

    def key(self, key):
        return self.recv_sems.at[self.keys.setdefault(key, len(self.keys))]

    def send(self, src, dst, to, key, group):
        number, total = self.groups.setdefault(group, (len(self.groups), []))
        total.append(math.prod(src.shape))
        pltpu.make_async_remote_copy(
            src_ref=src,
            dst_ref=dst,
            send_sem=self.send_sems.at[number],
            recv_sem=self.key(key),
            device_id=to,
            device_id_type=MESH,
        ).start()

    def of(self, ref, semaphore):
        return pltpu.make_async_remote_copy(
            src_ref=ref,
            dst_ref=ref,
            send_sem=semaphore,
            recv_sem=semaphore,
            device_id=self.anyone,
            device_id_type=MESH,
        )

    def wait(self, ref, key):
        self.of(ref, self.key(key)).wait_recv()

    def drain(self, sized):
        for number, total in self.groups.values():
            self.of(sized(sum(total)), self.send_sems.at[number]).wait_send()


def greet(p):
    barrier = pltpu.get_barrier_semaphore()
    friends = [p.xn, p.cn, p.zn["+"], p.zn["-"]]
    friends += [p.peer(p.other(o)) for o in range(1, p.copies)]
    for friend in friends:
        pl.semaphore_signal(barrier, inc=1, device_id=friend, device_id_type=MESH)
    pl.semaphore_wait(barrier, len(friends))


def hops_of(half):
    reach = {}
    for name in ("a1", "o"):
        reach["+", name], reach["-", name] = half, half - 1
    for name in ("a2", "t"):
        reach["+", name], reach["-", name] = half - 1, half
    return reach


NAMES = ("a1", "a2", "o", "t")


def gather(w, tag, full, p):
    q = full.shape[-1] // 4
    cols = {"a1": pl.ds(0, q), "a2": pl.ds(q, q), "o": pl.ds(2 * q, 2 * q), "t": pl.ds(2 * q, 2 * q)}
    reach = hops_of(p.half)
    whole = pl.ds(0, 4 * q)
    steps = []

    def piece(z, x, c, name):
        return full.at[p.block(z, x, c), :, whole if name == "all" else cols[name]]

    def put(z, x, name, to, key):
        ref = piece(z, x, p.c, name)
        w.send(ref, ref, to, key, (tag, "z" + key[1] if to is p.zn["+"] or to is p.zn["-"] else "x"))

    def share(z, x, name):
        ref = piece(z, x, p.c, name)
        w.send(ref, ref, p.cn, (tag, "c"), (tag, "c"))

    def own():
        put(p.z, p.x, "o", p.xn, (tag, "xb"))
        for name in ("a1", "a2", "o"):
            for way in "+-":
                put(p.z, p.x, name, p.zn[way], (tag, way, 1, name))
        for name in ("a1", "a2"):
            put(p.z, p.x, name, p.xn, (tag, "xa", "+", 0, name))
        share(p.z, p.x, "all")

    def crossed():
        w.wait(piece(p.z, 1 - p.x, p.c, "t"), (tag, "xb"))
        for way in "+-":
            put(p.z, 1 - p.x, "t", p.zn[way], (tag, way, 1, "t"))
        share(p.z, 1 - p.x, "t")

    def from_x(way, s, name):
        z = p.at(-s if way == "+" else s)
        w.wait(piece(z, 1 - p.x, p.c, name), (tag, "xa", way, s, name))
        share(z, 1 - p.x, name)

    def from_z(way, s, name):
        z = p.at(-s if way == "+" else s)
        x = 1 - p.x if name == "t" else p.x
        w.wait(piece(z, x, p.c, name), (tag, way, s, name))
        if s < reach[way, name]:
            put(z, x, name, p.zn[way], (tag, way, s + 1, name))
        if name in ("a1", "a2"):
            put(z, x, name, p.xn, (tag, "xa", way, s, name))
        share(z, x, name)

    def last():
        w.wait(full.at[pl.ds(0, 2 * p.deep)], (tag, "c"))

    steps += [own, crossed]
    steps += [functools.partial(from_x, "+", 0, name) for name in ("a1", "a2")]
    for s in range(1, p.half + 1):
        for name in NAMES:
            for way in "+-":
                if s <= reach[way, name]:
                    steps.append(functools.partial(from_z, way, s, name))
        for name in ("a1", "a2"):
            for way in "+-":
                if 1 <= s - 1 <= reach[way, name]:
                    steps.append(functools.partial(from_x, way, s - 1, name))
    for name in ("a1", "a2"):
        for way in "+-":
            if p.half <= reach[way, name]:
                steps.append(functools.partial(from_x, way, p.half, name))
    steps.append(last)
    return steps


def exchange(w, tag, src, spread, chosen, dst, pick, p):
    width = src.shape[-1] // p.copies

    def chunk(k):
        return pl.ds(pl.multiple_of(k * width, width), width)

    def out():
        for o in range(1, p.copies):
            k = p.other(o)
            w.send(src.at[:, chunk(k)], spread.at[p.replica], p.peer(k), (tag, "out"), (tag, "out"))
        spread[p.replica] = src[:, chunk(p.replica)]

    def through():
        w.wait(spread.at[pl.ds(0, p.copies - 1)], (tag, "out"))
        for o in range(1, p.copies):
            r = p.other(o)
            chosen[o] = spread[pick(r)]
            w.send(chosen.at[o], dst.at[:, chunk(p.replica)], p.peer(r), (tag, "back"), (tag, "back"))
        dst[:, chunk(p.replica)] = spread[pick(p.replica)]

    def back():
        w.wait(dst.at[:, pl.ds(0, (p.copies - 1) * width)], (tag, "back"))

    return [out, through, back]


def scatter(w, tag, part, got_c, put_x, got_x, put_z, got_z, put_b, got_b, p, finish):
    q = part.shape[-1] // 4
    a = pl.ds(0, 2 * q)
    cols = {"a1": pl.ds(0, q), "a2": pl.ds(q, q), "o": pl.ds(2 * q, 2 * q), "t": pl.ds(2 * q, 2 * q)}
    slot = {"a1": pl.ds(0, q), "a2": pl.ds(q, q), "o": pl.ds(2 * q, 2 * q), "t": pl.ds(4 * q, 2 * q)}
    reach = hops_of(p.half)
    index = {"+": 0, "-": 1}
    steps = []
    seen = set()

    def pair(z, x, where):
        return part[z, x, p.c, :, where].astype(F32) + got_c[z, x, :, where].astype(F32)

    def offsets(d):
        return (0,) if d == 0 else ((d,) if d == p.half else (d, -d))

    def halves():
        for d in range(p.half, -1, -1):
            for o in offsets(d):
                z = p.at(o)
                w.send(part.at[z, :, 1 - p.c], got_c.at[z], p.cn, (tag, "c", o), (tag, "c"))

    def cross(o):
        z = p.at(o)
        w.wait(got_c.at[z], (tag, "c", o))
        put_x[z] = pair(z, 1 - p.x, a).astype(BF)
        w.send(put_x.at[z], got_x.at[z], p.xn, (tag, "x", o), (tag, "x"))

    def value(z, name, where):
        x = 1 - p.x if name == "t" else p.x
        total = pair(z, x, where)
        if name in ("a1", "a2"):
            total += got_x[z, :, where].astype(F32)
        return total

    def arrived(o, name):
        if name in ("a1", "a2") and o not in seen:
            seen.add(o)
            w.wait(got_x.at[p.at(o)], (tag, "x", o))

    def came(way, d, name):
        ref = got_z.at[index[way], d - 1, :, slot[name]]
        w.wait(ref, (tag, way, d, name))
        return ref[...].astype(F32)

    def onward(way, d, name):
        o = d if way == "+" else (p.half if d == p.half else -d)
        z = p.at(o)
        arrived(o, name)
        total = value(z, name, cols[name])
        if d < reach[way, name]:
            total += came(way, d + 1, name)
        ref = put_z.at[index[way], d - 1, :, slot[name]]
        ref[...] = total.astype(BF)
        w.send(ref, got_z.at[index[way], d - 1, :, slot[name]], p.zn[way], (tag, way, d, name), (tag, "z" + way))

    def ended(name):
        arrived(0, name)
        total = value(p.z, name, cols[name])
        for way in "+-":
            if 1 <= reach[way, name]:
                total += came(way, 1, name)
        return total

    def hand():
        put_b[...] = ended("t").astype(BF)
        w.send(put_b, got_b, p.xn, (tag, "b"), (tag, "x"))
        finish(cols["a1"], ended("a1"))
        finish(cols["a2"], ended("a2"))

    def last():
        total = ended("o")
        w.wait(got_b, (tag, "b"))
        finish(cols["o"], total + got_b[...].astype(F32))

    def outward(d, names, fresh):
        return [
            functools.partial(onward, way, d, name)
            for name in names
            for way in "+-"
            if (d == reach[way, name] if fresh else d < reach[way, name])
        ]

    def crosses(d):
        return [functools.partial(cross, o) for o in offsets(d)] if d >= 0 else []

    top = p.half
    steps += [halves] + crosses(top) + outward(top, ("t", "o"), True)
    steps += crosses(top - 1) + outward(top - 1, ("t", "o"), True) + crosses(top - 2)
    steps += outward(top, ("a1", "a2"), True) + outward(top - 1, ("a1", "a2"), True)
    for d in range(top - 1, 0, -1):
        steps += outward(d, ("t", "a1", "a2"), False) + crosses(d - 2) + outward(d, ("o",), False)
    steps += [hand, last]
    return steps


def contract(left, right, left_dim, right_dim):
    return lax.dot_general(
        left, right, (((left_dim,), (right_dim,)), ((), ())), preferred_element_type=F32
    )


def mixed(steps, work):
    done = 0
    for k, step in enumerate(steps):
        step()
        while done < len(work) * (k + 1) // len(steps):
            work[done]()
            done += 1
    for piece in work[done:]:
        piece()


def forward(rows, pre, hidden, part, both_t, w_down):
    members, high, width = rows.shape
    q, units, lane = width // 4, hidden.shape[1], pre.shape[1] // 2
    count = members * high

    def grow(k):
        where = pl.ds(k * q, q)
        product = contract(rows[:, :, where].reshape(count, q), both_t[where, :], 1, 0)
        pre[...] = product if k == 0 else pre[...] + product

    def activate():
        gate = pre[:, pl.ds(0, units)]
        hidden[...] = (gate * jax.nn.sigmoid(gate) * pre[:, pl.ds(lane, units)]).astype(BF)

    def lower(k):
        where = pl.ds(k * q, q)
        product = contract(hidden[...], w_down[:, where], 1, 0).astype(BF)
        part[..., where] = product.reshape(part.shape[:-1] + (q,))

    work = [functools.partial(grow, k) for k in range(4)]
    return work + [activate] + [functools.partial(lower, k) for k in range(4)]


def kernel(sizes, scale, *refs):
    (
        partner, tokens, gate_in, up_in, down_in,
        rows_out, cot_out, hidden_t, d_both_t,
        full, cot, w_gate, w_up, w_down, both_t, pre, far_pre, hidden, far_hidden, slope_gate, slope_up, d_hidden,
        part, got_c, put_x, got_x, put_z, got_z, put_b, got_b,
        mine, taught, teacher, spread, chosen, spread_back, chosen_back, load_sems, send_sems, recv_sems,
    ) = refs
    p = Place(sizes)
    me = p.block(p.z, p.x, p.c)
    q = full.shape[-1] // 4
    load = pltpu.make_async_copy(tokens, full.at[me], load_sems.at[0])
    load.start()
    weights = [
        pltpu.make_async_copy(src, dst, load_sems.at[1 + k])
        for k, (src, dst) in enumerate(((gate_in, w_gate), (up_in, w_up), (down_in, w_down)))
    ]
    for copy in weights:
        copy.start()
    greet(p)
    load.wait()
    w = Wires(send_sems, recv_sems, p.cn)

    def taught_by(replica):
        found = jnp.int32(0)
        for r in range(p.copies):
            found = jnp.maximum(found, jnp.where(partner[r] == replica, jnp.int32(r), jnp.int32(0)))
        return found

    def keep_taught(where, value):
        taught[:, where] = value.astype(BF)

    def keep_mine(where, value):
        mine[:, where] = value

    rows_near, rows_far = (full.at[pl.ds(k * 4 * p.deep, 4 * p.deep)] for k in range(2))
    out, through, back = exchange(
        w, "e", rows_near.at[me], spread, chosen, rows_far.at[me], taught_by, p
    )
    near, far = gather(w, "s", rows_near, p), gather(w, "t", rows_far, p)
    near_work = forward(rows_near, pre, hidden, part.at[0], both_t, w_down)
    far_work = forward(rows_far, far_pre, far_hidden, part.at[1], both_t, w_down)
    near_sum, far_sum = (
        scatter(w, tag, *(r.at[k] for r in (part, got_c, put_x, got_x, put_z, got_z, put_b, got_b)), p, keep)
        for tag, k, keep in (("a", 0, keep_mine), ("b", 1, keep_taught))
    )
    back_out, back_through, back_back = exchange(
        w, "f", taught, spread_back, chosen_back, teacher, lambda r: partner[r], p
    )

    units, lane = hidden.shape[1], pre.shape[1] // 2

    def turn(src, dst, start, k):
        where = pl.ds(k * q, q)
        dst[where, pl.ds(start, units)] = src[:, where].T
        if lane > units:
            dst[where, pl.ds(start + units, lane - units)] = jnp.zeros((q, lane - units), BF)

    turns = [
        functools.partial(turn, src, dst, start, k)
        for src, dst, start in ((w_gate, both_t, 0), (w_up, both_t, lane))
        for k in range(4)
    ]
    near[0]()
    out()
    for copy in weights:
        copy.wait()
    mixed(turns, [])
    mixed(near[1:12], [])
    through()
    mixed(near[12:24], [])
    back()
    far[0]()
    mixed(near[24:34], [])
    mixed(far[1:4], [])
    mixed(near[34:-1], far[4:12])
    near[-1]()
    keep_rows = pltpu.make_async_copy(rows_near, rows_out, load_sems.at[4])
    keep_rows.start()
    mixed(far[12:], near_work)
    near_sum[0]()
    mixed(far_work, near_sum[1:EARLY])
    far_sum[0]()
    mixed(far_sum[1:9], [])
    mixed(far_sum[9:-2], near_sum[EARLY:LEAD])
    far_sum[-2]()
    mixed(near_sum[LEAD : LEAD + 3], [])
    far_sum[-1]()
    back_out()
    mixed(near_sum[LEAD + 3 : -LATE], [])
    back_through()
    mixed(near_sum[-LATE:], [])
    back_back()
    cot[me] = ((mine[...] - teacher[...].astype(F32)) * scale).astype(BF)
    count = pre.shape[0]

    def derive(k):
        here = pl.ds(k * 128, 128)
        gate, up = pre[here, pl.ds(0, units)], pre[here, pl.ds(lane, units)]
        sigma = jax.nn.sigmoid(gate)
        slope_gate[:, here] = (up * sigma * (1.0 + gate * (1.0 - sigma))).T
        slope_up[:, here] = (gate * sigma).T
        hidden_t[:, here] = hidden[here, :].T

    last = gather(w, "g", cot, p)
    last[0]()
    for k in range(count // 128):
        derive(k)
    mixed(last[1:], [])
    keep_cot = pltpu.make_async_copy(cot, cot_out, load_sems.at[5])
    keep_cot.start()
    for k in range(4):
        where = pl.ds(k * q, q)
        product = contract(w_down[:, where], cot[:, :, where].reshape(count, q), 1, 1)
        d_hidden[...] = product if k == 0 else d_hidden[...] + product
    d_both_t[pl.ds(0, units), :] = (d_hidden[...] * slope_gate[...]).astype(BF)
    d_both_t[pl.ds(units, units), :] = (d_hidden[...] * slope_up[...]).astype(BF)
    keep_cot.wait()

    def sized(elements):
        unit = full.shape[1] * q
        if elements % unit:
            return chosen.at[pl.ds(0, p.copies - 1)]
        return full.at[pl.ds(0, elements // unit), :, pl.ds(0, q)]

    keep_rows.wait()
    w.drain(sized)


def fused(sizes, scale, partner, tokens, w_gate, w_up, w_down):
    rows, width = tokens.shape
    units = w_gate.shape[0]
    lane = pl.cdiv(units, 128) * 128
    deep, members, copies = sizes["z"], sizes["z"] * 4, sizes["ry"] * sizes["rx"]
    half, q, count = deep // 2, width // 4, rows * members
    anywhere, vmem = pl.BlockSpec(memory_space=pl.ANY), pl.BlockSpec(memory_space=pltpu.VMEM)
    chunk = pltpu.VMEM((copies, rows, width // copies), BF)
    return pl.pallas_call(
        functools.partial(kernel, sizes, scale),
        out_shape=[
            jax.ShapeDtypeStruct((members, rows, width), BF),
            jax.ShapeDtypeStruct((members, rows, width), BF),
            jax.ShapeDtypeStruct((units, count), BF),
            jax.ShapeDtypeStruct((2 * units, count), BF),
        ],
        in_specs=[pl.BlockSpec(memory_space=pltpu.SMEM)] + [anywhere] * 4,
        out_specs=[anywhere] * 2 + [vmem] * 2,
        scratch_shapes=[
            pltpu.VMEM((2 * members, rows, width), BF),
            pltpu.VMEM((members, rows, width), BF),
            pltpu.VMEM((units, width), BF),
            pltpu.VMEM((units, width), BF),
            pltpu.VMEM((units, width), BF),
            pltpu.VMEM((width, 2 * lane), BF),
            pltpu.VMEM((count, 2 * lane), F32),
            pltpu.VMEM((count, 2 * lane), F32),
            pltpu.VMEM((count, units), BF),
            pltpu.VMEM((count, units), BF),
            pltpu.VMEM((units, count), F32),
            pltpu.VMEM((units, count), F32),
            pltpu.VMEM((units, count), F32),
            pltpu.VMEM((2, deep, 2, 2, rows, width), BF),
            pltpu.VMEM((2, deep, 2, rows, width), BF),
            pltpu.VMEM((2, deep, rows, 2 * q), BF),
            pltpu.VMEM((2, deep, rows, 2 * q), BF),
            pltpu.VMEM((2, 2, half, rows, 6 * q), BF),
            pltpu.VMEM((2, 2, half, rows, 6 * q), BF),
            pltpu.VMEM((2, rows, 2 * q), BF),
            pltpu.VMEM((2, rows, 2 * q), BF),
            pltpu.VMEM((rows, width), F32),
            pltpu.VMEM((rows, width), BF),
            pltpu.VMEM((rows, width), BF),
            chunk,
            chunk,
            chunk,
            chunk,
            pltpu.SemaphoreType.DMA((6,)),
            pltpu.SemaphoreType.DMA((NS,)),
            pltpu.SemaphoreType.DMA((NR,)),
        ],
        compiler_params=pltpu.CompilerParams(
            collective_id=0, has_side_effects=True, vmem_limit_bytes=62 * 1024 * 1024
        ),
        name="step",
    )(partner, tokens, w_gate, w_up, w_down)


def products_kernel(hidden_t, d_both_t, rows, cot, grad_gate, grad_up, grad_down):
    units = hidden_t.shape[0]
    both = contract(d_both_t[...], rows[...], 1, 0).astype(BF)
    grad_gate[...] = both[:units]
    grad_up[...] = both[units:]
    grad_down[...] = contract(hidden_t[...], cot[...], 1, 0).astype(BF)


def products(hidden_t, d_both_t, rows, cot):
    (units, count), width = hidden_t.shape, rows.shape[1]
    step = width // PARTS
    columns = pl.BlockSpec((count, step), lambda j: (0, j))
    return pl.pallas_call(
        products_kernel,
        grid=(PARTS,),
        out_shape=[jax.ShapeDtypeStruct((units, width), BF)] * 3,
        in_specs=[
            pl.BlockSpec((units, count), lambda j: (0, 0)),
            pl.BlockSpec((2 * units, count), lambda j: (0, 0)),
            columns,
            columns,
        ],
        out_specs=[pl.BlockSpec((units, step), lambda j: (0, j))] * 3,
        compiler_params=pltpu.CompilerParams(dimension_semantics=("arbitrary",)),
        name="products",
    )(hidden_t, d_both_t, rows, cot)


def local(sizes, partner, tokens, w_gate, w_up, w_down):
    rows, width = tokens.shape[1:]
    count = rows * sizes["z"] * 4
    scale = 1.0 / math.sqrt(count)
    rows_all, cot, hidden_t, d_both_t = fused(
        sizes, scale, partner, tokens[0], w_gate[0], w_up[0], w_down[0]
    )
    grads = products(hidden_t, d_both_t, rows_all.reshape(count, width), cot.reshape(count, width))
    return tuple(grad[None] for grad in grads)


def solution(mesh):
    members, copies = mesh.shape["fsdp"], mesh.shape["replica"]
    sizes = {"ry": copies // 2, "rx": 2, "z": members // 4, "x": 2, "c": 2}
    split = Mesh(mesh.devices.reshape(tuple(sizes.values())), tuple(sizes))
    spec = P(REPLICA, FSDP, None)
    return jax.shard_map(
        functools.partial(local, sizes),
        mesh=split,
        in_specs=(P(), spec, spec, spec, spec),
        out_specs=(spec, spec, spec),
        check_vma=False,
    )
```
